32 devices in a mesh: row: 4 (over y, x), col: 8 (over z, core).
Axes of the slice: x: 2, y: 2, z: 4, core: 2. Of those that a mesh axis runs over, the one named last changes fastest.
Arguments:
- inverse_factor: bfloat16 [8192, 8192], P('row', 'col'), may hold values from -1 to 2, as said below
- alpha_vector: float32 [8192], replicated, may hold values from -2 to 2
Outputs:
- weight_matrix: float32 [8192, 8192], P(('row', 'col'))
The draws below stay inside these ranges and needn't reach their ends.
Inputs may be any that keep to these rules, and one draw needn't show every extreme that they name: `inverse_factor`: lower triangular: every entry above the diagonal is zero; diagonal entries lie between 1 and 2.
All inputs are finite; a program needn't handle non-finite values.
Results may differ from the reference program's by a relative error of at most 0.0003.
Values may be sent and summed in bfloat16 or wider, within the bound.
A program may use at most 128 MiB of HBM per device.

```python
import jax
import jax.numpy as jnp

N = 8192


def draw_inverse_factor(key, part):
    first = jax.random.fold_in(key, 11)
    second = jax.random.fold_in(key, 23)
    spread = jnp.clip(jax.random.normal(first, (N, N), jnp.float32), -6.0, 6.0)
    diagonal = jnp.exp(jax.random.uniform(second, (N,), jnp.float32, 0.0, 0.6931472))
    lower = jnp.tril(spread * (2.0 / jnp.sqrt(jnp.float32(N))), -1)
    return (lower + jnp.diag(diagonal)).astype(jnp.bfloat16)


def bell_draw(key, dims, scale, bound, held_as=jnp.bfloat16):
    drawn = jax.random.normal(key, dims, jnp.float32) * scale
    return jnp.minimum(jnp.maximum(drawn, -bound), bound).astype(held_as)


def setup_inputs(seed: int = 0) -> dict:
    key_list = jax.random.split(jax.random.key(seed), 3)
    return {
        "inverse_factor": draw_inverse_factor(jax.random.fold_in(key_list[2], 71), 0),
        "alpha_vector": bell_draw(key_list[1], (N,), 0.3, 2.0, jnp.float32),
    }


def reference(inverse_factor, alpha_vector):
    gram = jnp.dot(inverse_factor.T, inverse_factor, preferred_element_type=jnp.float32)
    return gram - alpha_vector[:, None] * alpha_vector[None, :]
```

```python
import jax
import jax.numpy as jnp
from jax import lax
from jax.sharding import PartitionSpec as P


def contract(left, right):
    return lax.dot_general(
        left, right, (((0,), (0,)), ((), ())), preferred_element_type=jnp.float32
    )


def square_side(count):
    return max(side for side in range(1, count + 1) if count % side == 0 and side * side <= count)


def per_device(inverse_factor, alpha_vector):
    layer = lax.axis_index("row")
    column = lax.axis_index("col")
    n_row = lax.axis_size("row")
    n_col = lax.axis_size("col")
    tile_rows, tile_cols = inverse_factor.shape
    ratio = n_col // n_row
    width = tile_cols // n_row
    gathered = lax.all_gather(inverse_factor, "col", axis=0, tiled=False)
    block_in_layer = column * width // tile_cols
    first_col = column * width % tile_cols

    def owned_by(dest):
        start = (dest * ratio + block_in_layer, 0, first_col)
        return lax.dynamic_slice(gathered, start, (1, tile_rows, width))[0]

    sides = (n_row // square_side(n_row), square_side(n_row))
    place = (layer // sides[1], layer % sides[1])

    def index(first, second, order):
        return second * sides[1] + first if order else first * sides[1] + second

    def reduced(block, order):
        chunk = block // ratio
        n_first, n_second = (sides[1], sides[0]) if order else sides
        first, second = (place[1], place[0]) if order else place

        def dest(u, v, s, t):
            return index((u - s) % n_first, (v - t) % n_second, order)

        def partial_of(s, t):
            left = owned_by(dest(first, second, s, t))
            return contract(left, gathered[block])

        def owes(u, v, s, t):
            g = index(u, v, order)
            return g >= chunk and g >= dest(u, v, s, t)

        places = [(u, v) for u in range(n_first) for v in range(n_second)]

        def first_hop(s, t):
            pairs = [
                (index(u, v, order), dest(u, v, s, 0)) for u, v in places if owes(u, v, s, t)
            ]
            if not pairs:
                return None
            return lax.ppermute(partial_of(s, t).astype(jnp.float16), "row", pairs)

        def second_hop(value, t):
            pairs = []
            for u, v in places:
                if any(owes((u + s) % n_first, v, s, t) for s in range(n_first)):
                    pairs.append((index(u, v, order), dest(u, v, 0, t)))
            if not pairs:
                return None
            return lax.ppermute(value.astype(jnp.float16), "row", pairs)

        def add(total, part):
            return total if part is None else total + part.astype(jnp.float32)

        hops = {}
        for t in range(n_second - 1, -1, -1):
            for s in range(n_first - 1, 0, -1):
                hops[s, t] = first_hop(s, t)

        def finish():
            parts = []
            for t in range(n_second - 1, 0, -1):
                value = partial_of(0, t)
                for s in range(1, n_first):
                    value = add(value, hops[s, t])
                parts.append(second_hop(value, t))
            total = partial_of(0, 0)
            for s in range(1, n_first):
                total = add(total, hops[s, 0])
            for part in parts:
                total = add(total, part)
            return total

        return finish

    first_row = (layer * n_col + column) * width
    own_alpha = lax.dynamic_slice_in_dim(alpha_vector, first_row, width, 0)
    pieces = []
    for finish in [reduced(block, block % 2) for block in range(n_col)]:
        alpha = lax.slice_in_dim(
            alpha_vector, len(pieces) * tile_cols, (len(pieces) + 1) * tile_cols
        )
        pieces.append(finish() - own_alpha[:, None] * alpha[None, :])
    return jnp.concatenate(pieces, axis=1)


def solution(mesh):
    in_specs = (P("row", "col"), P())
    out_specs = P(("row", "col"), None)
    return jax.shard_map(
        per_device, mesh=mesh, in_specs=in_specs, out_specs=out_specs, check_vma=False
    )
```
